32 devices in a mesh: atom: 16 (over z, y, core), band: 2 (over x).
Axes of the slice: x: 2, y: 2, z: 4, core: 2. Of those that a mesh axis runs over, the one named last changes fastest.
Arguments:
- wave_rows: bfloat16 [256, 65536], P('atom', 'band'), may hold values from -6 to 6
- projectors: bfloat16 [2048, 65536], P('atom', 'band'), may hold values from -0.0234375 to 0.0234375
- dij_table: float32 [16, 8, 8], replicated, may hold values from -6 to 6
- dij_index: int32 [256], P('atom'), may hold values from 0 to 15
- proj_count: int32 [256], P('atom'), may hold values from 1 to 8
Outputs:
- nonlocal_rows: bfloat16 [256, 65536], P('atom', 'band')
The draws below stay inside these ranges and needn't reach their ends.
All inputs are finite; a program needn't handle non-finite values.
Results may differ from the reference program's by a relative error of at most 0.0049.
Values may be sent and summed in bfloat16 or wider, within the bound.
No kernel may reach another device: no remote copies, remote signals or barrier semaphores. Data moves between devices by JAX's collectives and lax.ppermute only.
A program may use at most 128 MiB of HBM per device.

```python
import jax
import jax.numpy as jnp
from jax import lax

G = 65536
PROJ = 8
KINDS = 16
ATOMS = 256
BANDS = 256


def touch_ends(entries, rng, smallest, high):
    extent = entries.shape
    index_at = [jax.random.randint(jax.random.fold_in(rng, axis), (), 0, extent[axis]) for axis in range(len(extent))]
    entries = entries.at[tuple(index_at)].set(smallest)
    longest = extent.index(max(extent))
    index_at[longest] = (index_at[longest] + 1) % extent[longest]
    return entries.at[tuple(index_at)].set(high)


def block_levels(own_key, dims, shards, smallest, high):
    loudness, own = 1.0, jax.random.fold_in(own_key, 6)
    for dim, parts in shards:
        heights = jnp.exp(jax.random.uniform(jax.random.fold_in(own, dim), (parts,), jnp.float32, smallest / len(shards), high / len(shards)))
        loudness = loudness * jnp.repeat(heights, dims[dim] // parts).reshape([-1 if axis == dim else 1 for axis in range(len(dims))])
    return loudness


def scatter_about(key, dims, width, limit, pieces=(), held_as=jnp.bfloat16):
    values = jax.random.normal(key, dims, jnp.float32) * width
    if len(pieces) > 0:
        values = block_levels(key, dims, pieces, -0.22, 0.18) * values
    return jnp.clip(values, min=-limit, max=limit).astype(held_as)


def setup_inputs(seed: int = 0) -> dict:
    key_list = jax.random.split(jax.random.key(seed), 6)
    return {
        "wave_rows": scatter_about(key_list[0], (BANDS, G), 1.0, 6.0, ((0, 16), (1, 2))),
        "projectors": scatter_about(key_list[1], (ATOMS * PROJ, G), G ** -0.5, 0.0234375, ((0, 16), (1, 2))),
        "dij_table": scatter_about(key_list[2], (KINDS, PROJ, PROJ), 1.0, 6.0, (), jnp.float32),
        "dij_index": touch_ends(jax.random.randint(key_list[3], (ATOMS,), 0, KINDS), jax.random.fold_in(key_list[3], 1), 0, KINDS - 1).astype(jnp.int32),
        "proj_count": touch_ends(jax.random.randint(key_list[4], (ATOMS,), 1, PROJ + 1), jax.random.fold_in(key_list[4], 1), 1, PROJ).astype(jnp.int32),
    }


def reference(wave_rows, projectors, dij_table, dij_index, proj_count):
    intersections = jnp.dot(wave_rows, projectors.T, preferred_element_type=jnp.float32)
    kind_onehot = (dij_index[:, None] == jnp.arange(KINDS, dtype=jnp.int32)[None, :]).astype(jnp.float32)
    blocks = jnp.dot(kind_onehot, dij_table.reshape(KINDS, PROJ * PROJ), precision=lax.Precision.HIGHEST).reshape(ATOMS, PROJ, PROJ)
    active = (jnp.arange(PROJ, dtype=jnp.int32)[None, :] < proj_count[:, None]).astype(jnp.float32)
    blocks = blocks * active[:, :, None] * active[:, None, :]
    weighted = jnp.einsum("baj,aij->bai", intersections.reshape(BANDS, ATOMS, PROJ), blocks, precision=lax.Precision.HIGHEST)
    weighted = weighted.reshape(BANDS, ATOMS * PROJ).astype(jnp.bfloat16)
    return jnp.dot(weighted, projectors, preferred_element_type=jnp.float32).astype(jnp.bfloat16)
```

```python
import jax
import jax.numpy as jnp
from jax import lax
from jax.sharding import Mesh
from jax.sharding import PartitionSpec as P


def block_diagonal(dij_table, dij_index, proj_count):
    atom_local = dij_index.shape[0]
    kind_total, per_atom = dij_table.shape[0], dij_table.shape[1]
    kind_onehot = (dij_index[:, None] == jnp.arange(kind_total, dtype=jnp.int32)[None, :]).astype(
        jnp.float32
    )
    blocks = jnp.dot(
        kind_onehot,
        dij_table.reshape(kind_total, per_atom * per_atom),
        precision=lax.Precision.HIGHEST,
    ).reshape(atom_local, per_atom, per_atom)
    active = (jnp.arange(per_atom, dtype=jnp.int32)[None, :] < proj_count[:, None]).astype(
        jnp.float32
    )
    blocks = blocks * active[:, :, None] * active[:, None, :]
    same = jnp.eye(atom_local, dtype=jnp.float32)
    spread = jnp.swapaxes(blocks, 1, 2)[:, :, None, :] * same[:, None, :, None]
    return spread.reshape(atom_local * per_atom, atom_local * per_atom)


def solution(mesh):
    atoms, bands = mesh.shape["atom"], mesh.shape["band"]
    lo = 4 if atoms % 4 == 0 else 1
    hi = atoms // lo
    grid = Mesh(mesh.devices.reshape(hi, lo, bands), ("hi", "lo", "band"))

    def swap(x, axis, size, step):
        return lax.ppermute(x, axis, [(k, k ^ step) for k in range(size)])

    def shift(x, step):
        return lax.ppermute(x, "hi", [(k, (k + step) % hi) for k in range(hi)])

    def shards(wave_rows, projectors, dij_table, dij_index, proj_count):
        rows, cols = wave_rows.shape
        span = cols // lo
        half = span // 2
        me = lax.axis_index("lo")

        def piece(x, step):
            return lax.dynamic_slice_in_dim(x, (me ^ step) * span, span, axis=1)

        parts = [piece(wave_rows, step) for step in range(lo)]
        for step in range(1, lo):
            parts[step] = swap(parts[step], "lo", lo, step)
        pieces = [piece(projectors, step) for step in range(lo)]
        wave_block = jnp.zeros((lo * rows, span), wave_rows.dtype)
        for step in range(lo):
            wave_block = lax.dynamic_update_slice_in_dim(
                wave_block, parts[step], (me ^ step) * rows, axis=0
            )
        proj = [pieces[0]]
        for step in range(1, lo):
            proj.append(swap(pieces[step], "lo", lo, step))
        stack = jnp.concatenate(proj, axis=0)
        group = lo * rows
        sides = []
        for side, way in ((0, 1), (1, -1)):
            block = wave_block[:, side * half : (side + 1) * half]
            whole = jnp.zeros((hi * group, half), wave_rows.dtype)
            whole = lax.dynamic_update_slice(whole, block, (0, 0))
            for t in range(1, hi):
                block = shift(block, way)
                whole = lax.dynamic_update_slice(whole, block, (way * t % hi * group, 0))
            sides.append(whole)

        def overlap(step):
            return sum(
                lax.dot_general(
                    sides[side],
                    proj[step][:, side * half : (side + 1) * half],
                    (((1,), (1,)), ((), ())),
                    preferred_element_type=jnp.float32,
                )
                for side in range(2)
            )

        total = overlap(0)
        for step in range(1, lo):
            total = total + swap(overlap(step), "lo", lo, step)
        if bands & (bands - 1) == 0:
            step = 1
            while step < bands:
                total = total + swap(total, "band", bands, step)
                step *= 2
        else:
            total = lax.psum(total, "band")
        mixed = jnp.dot(
            total,
            block_diagonal(dij_table, dij_index, proj_count),
            precision=lax.Precision.HIGHEST,
        ).astype(jnp.bfloat16)
        weighted = jnp.concatenate(
            [mixed] + [swap(mixed, "lo", lo, step) for step in range(1, lo)], axis=1
        )

        quarter = half // 2

        def contribution(r, side, sub):
            at = side * half + sub * quarter
            return jnp.dot(
                weighted[r * group : (r + 1) * group],
                stack[:, at : at + quarter],
                preferred_element_type=jnp.float32,
            )

        streams = [(sub, side, 1 - 2 * side) for sub in range(2) for side in range(2)]
        acc = [contribution(way % hi, side, sub) for sub, side, way in streams]
        for t in range(1, hi):
            moved = []
            for a, (sub, side, way) in zip(acc, streams):
                moved.append(shift(a.astype(jnp.bfloat16), way))
            acc = [
                contribution(way * (1 + t) % hi, side, sub) + m.astype(jnp.float32)
                for m, (sub, side, way) in zip(moved, streams)
            ]
        acc = [a.astype(jnp.bfloat16) for a in acc]
        result = jnp.zeros((rows, cols), jnp.bfloat16)
        for sub in range(2):
            own = jnp.concatenate(acc[2 * sub : 2 * sub + 2], axis=1)
            for step in range(lo):
                part = lax.dynamic_slice_in_dim(own, (me ^ step) * rows, rows, axis=0)
                if step:
                    part = swap(part, "lo", lo, step)
                for side in range(2):
                    result = lax.dynamic_update_slice_in_dim(
                        result,
                        part[:, side * quarter : (side + 1) * quarter],
                        (me ^ step) * span + side * half + sub * quarter,
                        axis=1,
                    )
        return result

    spec = P(("hi", "lo"), "band")
    index_spec = P(("hi", "lo"))

    return jax.shard_map(
        shards,
        mesh=grid,
        in_specs=(spec, spec, P(), index_spec, index_spec),
        out_specs=spec,
        check_vma=False,
    )
```
